32 devices in a mesh: row: 4 (over y, core), col: 8 (over z, x).
Axes of the slice: x: 2, y: 2, z: 4, core: 2. Of those that a mesh axis runs over, the one named last changes fastest.
Arguments:
- residual: bfloat16 [1024, 8192], P('row', 'col'), may hold values from -6 to 6
- strip_weights: bfloat16 [1024, 512], P('row'), may hold values from -0.375 to 0.375
- bin_weights: bfloat16 [4, 8192, 1024], P('row', 'col'), may hold values from -0.25 to 0.25
- touched: int32 [4, 8, 8], P('row', 'col'), may hold values 0 or 1
- image: float32 [2048, 1024], P('row', 'col'), may hold values from -6 to 6
- precond: float32 [2048, 1024], P('row', 'col'), may hold values from 0.05 to 1.35, as said below
Outputs:
- updated: float32 [2048, 1024], P('row', 'col')
- mean_change: float32 [], replicated
The draws below stay inside these ranges and needn't reach their ends.
Inputs may be any that keep to these rules, and one draw needn't show every extreme that they name: `precond`: positive.
All inputs are finite; a program needn't handle non-finite values. No bound on the sum of `touched` on one device may be relied on, other than what follows from the above.
Results may differ from the reference program's by a relative error of at most 0.0023.
Values sent between devices are 32-bit elements; how exact they have to be, the bound alone decides.
A program may use at most 64 MiB of HBM per device.

```python
import jax
import jax.numpy as jnp
from jax import lax

TILE_R = 512
TILE_C = 128
ANG = 256
DB = 1024
ITERS = 10
IMAGE_R = 2048
IMAGE_C = 1024
N_ROW = 4
N_COL = 8


def draw_precond(key, part):
    row_pos = lax.broadcasted_iota(jnp.float32, (IMAGE_R, IMAGE_C), 0) / (IMAGE_R - 1)
    col_pos = lax.broadcasted_iota(jnp.float32, (IMAGE_R, IMAGE_C), 1) / (IMAGE_C - 1)
    uniform_part = jax.random.uniform(key, (IMAGE_R, IMAGE_C), jnp.float32)
    base = 0.05 * jnp.exp(uniform_part * jnp.log(3.0))
    ramp = (1.0 + 2.0 * row_pos) * (1.0 + 2.0 * col_pos)
    return (base * ramp).astype(jnp.float32)


def with_ends(values, rng, low, high):
    longest = values.shape.index(max(values.shape))
    spots = []
    for shift in (0, 1):
        where = [jax.random.randint(jax.random.fold_in(rng, axis), (), 0, length) for axis, length in enumerate(values.shape)]
        where[longest] = (where[longest] + shift) % values.shape[longest]
        spots.append(tuple(where))
    return values.at[spots[0]].set(low).at[spots[1]].set(high)


def spiked(values, rng, source, target, shards_of, factor):
    def block_of(axis_at):
        return (jnp.arange(values.shape[axis_at]) // (values.shape[axis_at] // shards_of)).reshape((-1,) + (1,) * (values.ndim - 1 - axis_at))

    near = jax.random.permutation(rng, shards_of)[block_of(target)]
    second = (block_of(target) + shards_of // 2) % shards_of
    return jnp.where((block_of(source) == near) | (block_of(source) == second), factor * values, values)


def level_of(rng, extent, cuts, low, high):
    def one(dim, blocks):
        draws = jax.random.uniform(jax.random.fold_in(jax.random.fold_in(rng, 6), dim), (blocks,), jnp.float32, low / len(cuts), high / len(cuts))
        return jnp.repeat(jnp.exp(draws), extent[dim] // blocks).reshape((-1,) + (1,) * (len(extent) - dim - 1))

    gain = one(*cuts[0])
    for cut in cuts[1:]:
        gain = gain * one(*cut)
    return gain


def scatter_about(own_key, dims, deviation, most, split=(), held_as=jnp.bfloat16):
    values = jax.random.normal(own_key, dims, jnp.float32) * deviation
    if len(split) > 0:
        values = level_of(own_key, dims, split, -0.22, 0.18) * values
    return jnp.clip(values, min=-most, max=most).astype(held_as)


def noise_with(stream_key, dims, deviation, bound, split, heavy, kind=jnp.bfloat16):
    values = deviation * jax.random.normal(stream_key, dims, jnp.float32)
    if split:
        values = values * level_of(stream_key, dims, split, -0.22, 0.18)
    return jnp.clip(spiked(values, jax.random.fold_in(stream_key, 3), *heavy), -bound, bound).astype(kind)


def setup_inputs(seed: int = 0) -> dict:
    streams_of = jax.random.split(jax.random.key(seed), 7)
    residual = scatter_about(streams_of[0], (N_ROW * ANG, N_COL * DB), 1.0, 6.0, ((0, 4), (1, 8)))
    strip_weights = scatter_about(streams_of[1], (N_ROW * ANG, TILE_R), ANG ** -0.5, 0.375, ((0, 4),))
    bin_weights = noise_with(streams_of[2], (N_ROW, N_COL * DB, IMAGE_C), DB ** -0.5, 0.25, ((0, 4), (1, 8)), (1, 2, 8, 2.0))
    touched = with_ends((jax.random.randint(streams_of[3], (N_ROW, N_COL, N_COL), 0, 4) < 3).astype(jnp.int32), jax.random.fold_in(streams_of[3], 1), 0, 1)
    image = scatter_about(streams_of[4], (IMAGE_R, IMAGE_C), 1.0, 6.0, ((0, 4), (1, 8)), jnp.float32)
    precond = draw_precond(jax.random.fold_in(streams_of[6], 71), 0)
    return {"residual": residual, "strip_weights": strip_weights, "bin_weights": bin_weights, "touched": touched, "image": image, "precond": precond}


tv_weight = 0.25
dual_step = 0.125
radius = 0.25
epsilon = 1e-06

def divergence(down, right):
    above = jnp.concatenate([jnp.zeros_like(down[:1]), down[:-1]], 0)
    beside = jnp.concatenate([jnp.zeros_like(right[:, :1]), right[:, :-1]], 1)
    return down - above + (right - beside)

def reference(residual, strip_weights, bin_weights, touched, image, precond):
    strips = []
    for strip_index in range(N_ROW):
        sinogram = residual[strip_index * ANG:(strip_index + 1) * ANG]
        sinogram = jnp.transpose(sinogram.reshape(ANG, N_COL, DB), (1, 0, 2))
        weights = bin_weights[strip_index].reshape(N_COL, DB, IMAGE_C)
        marks = touched[strip_index].astype(jnp.float32)

        def add_block(running, pieces):
            sino_block, weight_block, tile_marks = pieces
            product = jnp.dot(sino_block, weight_block, preferred_element_type=jnp.float32)
            product = product.reshape(ANG, N_COL, TILE_C) * tile_marks[None, :, None]
            return (running + product, None)
        summed, _unused = lax.scan(add_block, jnp.zeros((ANG, N_COL, TILE_C), jnp.float32), (sinogram, weights, marks))
        factor_block = strip_weights[strip_index * ANG:(strip_index + 1) * ANG].astype(jnp.float32)
        strip = jnp.einsum('ar,act->rct', factor_block, summed, precision=lax.Precision.HIGHEST)
        strips.append(strip.reshape(TILE_R, IMAGE_C))
    gradient = jnp.concatenate(strips, 0)
    step_dir = precond * gradient
    spread = jnp.sqrt(jnp.sum(step_dir * step_dir) / (IMAGE_R * IMAGE_C) + epsilon)
    factor = jnp.minimum(1.0, radius / spread)
    source = image - factor * step_dir
    scaled = source / tv_weight
    down = jnp.zeros_like(source)
    right = jnp.zeros_like(source)
    for turn_index in range(ITERS):
        potential = divergence(down, right) - scaled
        grad_down = jnp.concatenate([potential[1:] - potential[:-1], jnp.zeros_like(potential[:1])], 0)
        grad_right = jnp.concatenate([potential[:, 1:] - potential[:, :-1], jnp.zeros_like(potential[:, :1])], 1)
        magnitude = jnp.sqrt(grad_down * grad_down + grad_right * grad_right)
        divisor = 1.0 + dual_step * magnitude
        down = (down + dual_step * grad_down) / divisor
        right = (right + dual_step * grad_right) / divisor
    updated = source - tv_weight * divergence(down, right)
    change = updated - image
    mean_change = jnp.sum(change * change) / (IMAGE_R * IMAGE_C)
    return (updated, mean_change)
```

```python
import functools

import jax
import jax.numpy as jnp
from jax import lax
from jax.experimental import pallas as pl
from jax.experimental.pallas import tpu as pltpu
from jax.sharding import PartitionSpec as P

ITERS = 10
LANES = 128
HALO = 16
PAD = 8
BASE = PAD + HALO

tv_weight = 0.25
dual_step = 0.125
radius = 0.25
epsilon = 1e-06


def kernel(
    n_row, n_col,
    res_ref, strip_ref, bin_ref, touched_ref, image_ref, precond_ref,
    out_ref, mean_ref,
    prod, recv1, send2, recv2,
    img_t, step_t, halo_img, halo_step, strips, prec_t,
    p_ref, q_ref, pot_ref, scaled_ref, mask_d, mask_r,
    sq_row, sq_col, ch_row, ch_col,
    s1, r1, s2, r2,
    img_send, img_recv, step_send, step_recv,
    sq_row_s, sq_row_r, sq_col_s, sq_col_r,
    ch_row_s, ch_row_r, ch_col_s, ch_col_r,
):
    tile_rows, tile_cols = image_ref.shape
    tiles = tile_rows // LANES
    me_r = lax.axis_index("row")
    me_c = lax.axis_index("col")
    groups = n_col // 2
    g = me_c // 2
    b = lax.rem(me_c, 2)
    peer = 2 * g + 1 - b
    total_rows = n_row * tile_rows
    total_cols = n_col * tile_cols
    cell_total = float(total_rows * total_cols)
    main = pl.ds(BASE, tile_cols)

    for ref in (img_t, step_t, halo_img, halo_step, p_ref, q_ref, pot_ref):
        ref[...] = jnp.zeros_like(ref)

    barrier = pltpu.get_barrier_semaphore()
    for d in range(1, n_col):
        pl.semaphore_signal(barrier, inc=1, device_id={"col": lax.rem(me_c + d, n_col)})
    for d in range(1, n_row):
        pl.semaphore_signal(barrier, inc=1, device_id={"row": lax.rem(me_r + d, n_row)})
    pl.semaphore_wait(barrier, n_col - 1 + n_row - 1)

    def remote(src, dst, send, recv, **where):
        return pltpu.make_async_remote_copy(
            src_ref=src, dst_ref=dst, send_sem=send, recv_sem=recv, device_id=where
        )

    up_ok, down_ok = me_r > 0, me_r < n_row - 1
    left_ok, right_ok = me_c > 0, me_c < n_col - 1

    def row_copies(top, bottom, halo, send, recv):
        up = remote(top, halo.at[pl.ds(0, HALO)], send.at[0], recv.at[0], row=jnp.maximum(me_r - 1, 0))
        down = remote(
            bottom, halo.at[pl.ds(LANES - HALO, HALO)], send.at[1], recv.at[1],
            row=jnp.minimum(me_r + 1, n_row - 1),
        )
        return up, down

    def col_copies(field, first, count, at, send, recv):
        span = pl.ds(first, count)
        left = remote(
            field.at[span, pl.ds(BASE, HALO)], field.at[span, pl.ds(BASE + tile_cols, HALO)],
            send.at[at], recv.at[at], col=jnp.maximum(me_c - 1, 0),
        )
        right = remote(
            field.at[span, pl.ds(BASE + tile_cols - HALO, HALO)], field.at[span, pl.ds(PAD, HALO)],
            send.at[at + 1], recv.at[at + 1], col=jnp.minimum(me_c + 1, n_col - 1),
        )
        return left, right

    def start(pair, first_ok, second_ok):
        pl.when(first_ok)(lambda: pair[0].start())
        pl.when(second_ok)(lambda: pair[1].start())

    def wait_recv(pair, first_ok, second_ok):
        pl.when(second_ok)(lambda: pair[0].wait_recv())
        pl.when(first_ok)(lambda: pair[1].wait_recv())

    def wait_send(pair, first_ok, second_ok):
        pl.when(first_ok)(lambda: pair[0].wait_send())
        pl.when(second_ok)(lambda: pair[1].wait_send())

    order = sorted(range(1, groups), key=lambda d: -min(d, groups - d)) + [0]
    firsts = {}
    for d in order:
        to = lax.rem(g + d, groups)
        cols = pl.ds(pl.multiple_of(to * (2 * tile_cols), 2 * tile_cols), 2 * tile_cols)
        product = jnp.dot(res_ref[...], bin_ref[0, :, cols], preferred_element_type=jnp.float32)
        for h in range(2):
            mark = touched_ref[0, 0, 2 * to + h].astype(jnp.float32)
            prod[2 * to + h] = product[:, h * tile_cols:(h + 1) * tile_cols] * mark
        firsts[d] = remote(prod.at[2 * to + 1 - b], recv1.at[to], s1.at[to], r1.at[to], col=peer)
        firsts[d].start()

    img_rows = row_copies(
        image_ref.at[pl.ds(0, HALO)], image_ref.at[pl.ds(tile_rows - HALO, HALO)],
        halo_img, img_send, img_recv,
    )
    start(img_rows, up_ok, down_ok)
    for j in range(tiles):
        rows = pl.ds(j * LANES, LANES)
        img_t[j, main, :] = image_ref[rows, :].T
        prec_t[j] = precond_ref[rows, :].T
    img_cols = col_copies(img_t, 0, tiles, 2, img_send, img_recv)
    start(img_cols, left_ok, right_ok)

    strip_top = strip_ref[:, :LANES].astype(jnp.float32).T[:HALO]
    strip_bottom = strip_ref[:, tile_rows - LANES:].astype(jnp.float32).T[LANES - HALO:]
    strip_edges = jnp.concatenate([strip_top, strip_bottom], 0).astype(jnp.bfloat16)

    depth = img_t.shape[1]
    lane = lax.broadcasted_iota(jnp.int32, (depth, LANES), 1)
    col_ids = me_c * tile_cols - BASE + lax.broadcasted_iota(jnp.int32, (depth, LANES), 0)
    for j in range(tiles + 1):
        if j < tiles:
            row_ids = me_r * tile_rows + j * LANES + lane
        else:
            row_ids = me_r * tile_rows + jnp.where(lane < LANES // 2, tile_rows + lane, lane - LANES)
        inside = (row_ids >= 0) & (row_ids < total_rows) & (col_ids >= 0) & (col_ids < total_cols)
        mask_d[j] = jnp.where(inside & (row_ids < total_rows - 1), dual_step, 0.0)
        mask_r[j] = jnp.where(inside & (col_ids < total_cols - 1), dual_step, 0.0)

    seconds = []
    for d in order:
        to = lax.rem(g + d, groups)
        firsts[d].wait_recv()
        if d:
            send2[to] = prod[2 * to + b] + recv1[to]
            copy = remote(send2.at[to], recv2.at[g], s2.at[to], r2.at[g], col=2 * to + b)
            copy.start()
            seconds.append(copy)

    wait_recv(img_rows, up_ok, down_ok)
    img_t[tiles, main, :] = halo_img[...].T
    img_corner = col_copies(img_t, tiles, 1, 4, img_send, img_recv)
    start(img_corner, left_ok, right_ok)

    sums = prod[2 * g + b] + recv1[g]
    for d in order[:-1]:
        sender = lax.rem(g - d + groups, groups)
        remote(send2.at[sender], recv2.at[sender], s2.at[sender], r2.at[sender], col=peer).wait_recv()
        sums = sums + recv2[sender]

    def parts(x):
        high = x.astype(jnp.bfloat16)
        return high, (x - high.astype(jnp.float32)).astype(jnp.bfloat16)

    high, low = parts(sums)
    edges = jnp.dot(strip_edges, high, preferred_element_type=jnp.float32)
    edges = edges + jnp.dot(strip_edges, low, preferred_element_type=jnp.float32)
    strips[pl.ds(0, HALO), :] = edges[:HALO] * precond_ref[pl.ds(0, HALO), :]
    strips[pl.ds(HALO, HALO), :] = edges[HALO:] * precond_ref[pl.ds(tile_rows - HALO, HALO), :]
    step_rows = row_copies(
        strips.at[pl.ds(0, HALO)], strips.at[pl.ds(HALO, HALO)], halo_step, step_send, step_recv
    )
    start(step_rows, up_ok, down_ok)

    high, low = parts(sums.T)
    square = jnp.zeros((8, LANES), jnp.float32)
    for j in range(tiles):
        weights = strip_ref[:, j * LANES:(j + 1) * LANES]
        grad = jnp.dot(high, weights, preferred_element_type=jnp.float32)
        grad = grad + jnp.dot(low, weights, preferred_element_type=jnp.float32)
        step = prec_t[j] * grad
        step_t[j, main, :] = step
        square = square + jnp.sum((step * step).reshape(tile_cols // 8, 8, LANES), 0)

    def spread_over(value, slots, mine, count, axis, send, recv):
        slots[mine] = value
        copies = []
        for d in range(1, count):
            to = lax.rem(mine + d, count)
            copy = remote(slots.at[mine], slots.at[mine], send.at[to], recv.at[mine], **{axis: to})
            copy.start()
            copies.append(copy)
        return copies

    def collected(slots, mine, count, axis, send, recv):
        for d in range(1, count):
            at = lax.rem(mine + d, count)
            remote(slots.at[at], slots.at[at], send.at[at], recv.at[at], **{axis: at}).wait_recv()
        total = slots[0]
        for i in range(1, count):
            total = total + slots[i]
        return total

    pending = spread_over(square, sq_row, me_r, n_row, "row", sq_row_s, sq_row_r)
    step_cols = col_copies(step_t, 0, tiles, 2, step_send, step_recv)
    start(step_cols, left_ok, right_ok)
    wait_recv(step_rows, up_ok, down_ok)
    step_t[tiles, main, :] = halo_step[...].T
    step_corner = col_copies(step_t, tiles, 1, 4, step_send, step_recv)
    start(step_corner, left_ok, right_ok)
    square = collected(sq_row, me_r, n_row, "row", sq_row_s, sq_row_r)
    pending += spread_over(square, sq_col, me_c, n_col, "col", sq_col_s, sq_col_r)
    for pair in (img_cols, img_corner, step_cols, step_corner):
        wait_recv(pair, left_ok, right_ok)
    square = collected(sq_col, me_c, n_col, "col", sq_col_s, sq_col_r)
    spread = jnp.sqrt(jnp.sum(square, axis=(0, 1), keepdims=True) / cell_total + epsilon)
    factor = jnp.minimum(1.0, radius / spread)
    factor = jnp.broadcast_to(factor, (depth, LANES))
    for j in range(tiles + 1):
        scaled_ref[j] = (img_t[j] - factor * step_t[j]) / tv_weight

    def turned(pieces, shift):
        rolled = [pltpu.roll(piece, shift % LANES, 1) for piece in pieces]
        at = lax.broadcasted_iota(jnp.int32, pieces[0].shape, 1)
        edge = at == (0 if shift > 0 else LANES - 1)
        n = len(pieces)
        return [jnp.where(edge, rolled[(i - shift) % n], rolled[i]) for i in range(n)]

    every = range(tiles + 1)

    def divergence(first, size, count=tiles + 1):
        p = [p_ref[j, pl.ds(first, size), :] for j in every]
        above = turned(p, 1)
        q = [q_ref[j, pl.ds(first, size), :] for j in range(count)]
        beside = [q_ref[j, pl.ds(first - 1, size), :] for j in range(count)]
        return [p[j] - above[j] + (q[j] - beside[j]) for j in range(count)]

    CHUNK = 16

    def turn(low_end, high_end):
        for first in range(low_end, high_end, CHUNK):
            div = divergence(first, CHUNK)
            for j in every:
                pot_ref[j, pl.ds(first, CHUNK), :] = div[j] - scaled_ref[j, pl.ds(first, CHUNK), :]
        for first in range(low_end, high_end, CHUNK):
            here = pl.ds(first, CHUNK)
            pot = [pot_ref[j, here, :] for j in every]
            below = turned(pot, -1)
            for j in every:
                grad_d = (below[j] - pot[j]) * mask_d[j, here, :]
                grad_r = (pot_ref[j, pl.ds(first + 1, CHUNK), :] - pot[j]) * mask_r[j, here, :]
                inverse = 1.0 / (1.0 + jnp.sqrt(grad_d * grad_d + grad_r * grad_r))
                p_ref[j, here, :] = (p_ref[j, here, :] + grad_d) * inverse
                q_ref[j, here, :] = (q_ref[j, here, :] + grad_r) * inverse

    wide = max(0, ITERS - PAD)

    @pl.loop(0, wide)
    def _(_):
        turn(PAD, depth - PAD)

    @pl.loop(wide, ITERS)
    def _(_):
        turn(HALO, depth - HALO)

    moved = jnp.zeros((8, LANES), jnp.float32)
    for first in range(BASE, BASE + tile_cols, CHUNK):
        div = divergence(first, CHUNK, tiles)
        for j in range(tiles):
            here = pl.ds(first, CHUNK)
            updated = tv_weight * (scaled_ref[j, here, :] - div[j])
            pot_ref[j, here, :] = updated
            change = updated - img_t[j, here, :]
            moved = moved + jnp.sum((change * change).reshape(CHUNK // 8, 8, LANES), 0)
    pending += spread_over(moved, ch_row, me_r, n_row, "row", ch_row_s, ch_row_r)
    moved = collected(ch_row, me_r, n_row, "row", ch_row_s, ch_row_r)
    pending += spread_over(moved, ch_col, me_c, n_col, "col", ch_col_s, ch_col_r)
    for j in range(tiles):
        out_ref[pl.ds(j * LANES, LANES), :] = pot_ref[j, main, :].T
    for d in order:
        firsts[d].wait_send()
    for copy in seconds:
        copy.wait_send()
    for pair in (img_rows, step_rows):
        wait_send(pair, up_ok, down_ok)
    for pair in (img_cols, img_corner, step_cols, step_corner):
        wait_send(pair, left_ok, right_ok)
    moved = collected(ch_col, me_c, n_col, "col", ch_col_s, ch_col_r)
    mean_ref[0] = jnp.sum(moved) / cell_total
    for copy in pending:
        copy.wait_send()


def solution(mesh):
    n_row, n_col = mesh.shape["row"], mesh.shape["col"]

    def local(residual, strip_weights, bin_weights, touched, image, precond):
        angles = residual.shape[0]
        tile_rows, tile_cols = image.shape
        tiles = tile_rows // LANES
        depth = tile_cols + 2 * BASE
        groups = n_col // 2
        f32 = jnp.float32
        vmem = pl.BlockSpec(memory_space=pltpu.VMEM)
        smem = pl.BlockSpec(memory_space=pltpu.SMEM)
        dma = pltpu.SemaphoreType.DMA
        field = pltpu.VMEM((tiles + 1, depth, LANES), f32)
        strip = pltpu.VMEM((LANES, tile_cols), f32)
        updated, mean_change = pl.pallas_call(
            functools.partial(kernel, n_row, n_col),
            out_shape=(
                jax.ShapeDtypeStruct(image.shape, f32),
                jax.ShapeDtypeStruct((1,), f32),
            ),
            in_specs=[vmem, vmem, vmem, smem, vmem, vmem],
            out_specs=(vmem, smem),
            scratch_shapes=[
                pltpu.VMEM((n_col, angles, tile_cols), f32),
                pltpu.VMEM((groups, angles, tile_cols), f32),
                pltpu.VMEM((groups, angles, tile_cols), f32),
                pltpu.VMEM((groups, angles, tile_cols), f32),
                field, field, strip, strip,
                pltpu.VMEM((2 * HALO, tile_cols), f32),
                pltpu.VMEM((tiles, tile_cols, LANES), f32),
                field, field, field, field, field, field,
                pltpu.VMEM((n_row, 8, LANES), f32),
                pltpu.VMEM((n_col, 8, LANES), f32),
                pltpu.VMEM((n_row, 8, LANES), f32),
                pltpu.VMEM((n_col, 8, LANES), f32),
                dma((groups,)), dma((groups,)), dma((groups,)), dma((groups,)),
                dma((6,)), dma((6,)), dma((6,)), dma((6,)),
                dma((n_row,)), dma((n_row,)), dma((n_col,)), dma((n_col,)),
                dma((n_row,)), dma((n_row,)), dma((n_col,)), dma((n_col,)),
            ],
            compiler_params=pltpu.CompilerParams(collective_id=0, has_side_effects=True),
            name="tv_step",
        )(residual, strip_weights, bin_weights, touched, image, precond)
        return updated, mean_change.reshape(())

    in_specs = (
        P("row", "col"),
        P("row", None),
        P("row", "col", None),
        P("row", "col", None),
        P("row", "col"),
        P("row", "col"),
    )
    return jax.shard_map(
        local, mesh=mesh, in_specs=in_specs, out_specs=(P("row", "col"), P()), check_vma=False
    )
```

```python
import functools

import jax
import jax.numpy as jnp
from jax import lax
from jax.experimental import pallas as pl
from jax.experimental.pallas import tpu as pltpu
from jax.sharding import PartitionSpec as P

ITERS = 10
LANES = 128
HALO = 16
PAD = 8
BASE = PAD + HALO

tv_weight = 0.25
dual_step = 0.125
radius = 0.25
epsilon = 1e-06


def kernel(
    n_row, n_col,
    res_ref, strip_ref, bin_ref, touched_ref, image_ref, precond_ref,
    out_ref, mean_ref,
    prod, recv1, send2, recv2,
    img_t, step_t, halo_img, halo_step, strips, prec_t,
    p_ref, q_ref, pot_ref, scaled_ref, mask_d, mask_r,
    sq_row, sq_col, ch_row, ch_col,
    s1, r1, s2, r2, bins, bins_sem,
    img_send, img_recv, step_send, step_recv,
    sq_row_s, sq_row_r, sq_col_s, sq_col_r,
    ch_row_s, ch_row_r, ch_col_s, ch_col_r,
):
    tile_rows, tile_cols = image_ref.shape
    tiles = tile_rows // LANES
    me_r = lax.axis_index("row")
    me_c = lax.axis_index("col")
    groups = n_col // 2
    g = me_c // 2
    b = lax.rem(me_c, 2)
    peer = 2 * g + 1 - b
    total_rows = n_row * tile_rows
    total_cols = n_col * tile_cols
    cell_total = float(total_rows * total_cols)
    main = pl.ds(BASE, tile_cols)

    order = [groups // 2] if groups > 1 else []
    for i in range((groups - 1) // 2, 0, -1):
        order += [-i, i]
    order.append(0)
    mirror = 1 - 2 * lax.rem(g, 2)
    targets = [lax.rem(g + mirror * d + groups, groups) for d in order]
    loads = []
    for k, to in enumerate(targets):
        cols = pl.ds(pl.multiple_of(to * (2 * tile_cols), 2 * tile_cols), 2 * tile_cols)
        loads.append(pltpu.make_async_copy(bin_ref.at[0, :, cols], bins.at[k], bins_sem.at[k]))
        loads[k].start()

    for ref in (img_t, step_t, halo_img, halo_step, p_ref, q_ref, pot_ref):
        ref[...] = jnp.zeros_like(ref)

    barrier = pltpu.get_barrier_semaphore()
    for d in range(1, n_col):
        pl.semaphore_signal(barrier, inc=1, device_id={"col": lax.rem(me_c + d, n_col)})
    for d in range(1, n_row):
        pl.semaphore_signal(barrier, inc=1, device_id={"row": lax.rem(me_r + d, n_row)})

    def remote(src, dst, send, recv, **where):
        return pltpu.make_async_remote_copy(
            src_ref=src, dst_ref=dst, send_sem=send, recv_sem=recv, device_id=where
        )

    up_ok, down_ok = me_r > 0, me_r < n_row - 1
    left_ok, right_ok = me_c > 0, me_c < n_col - 1

    def row_copies(top, bottom, halo, send, recv):
        up = remote(top, halo.at[pl.ds(0, HALO)], send.at[0], recv.at[0], row=jnp.maximum(me_r - 1, 0))
        down = remote(
            bottom, halo.at[pl.ds(LANES - HALO, HALO)], send.at[1], recv.at[1],
            row=jnp.minimum(me_r + 1, n_row - 1),
        )
        return up, down

    def col_copies(field, first, count, at, send, recv):
        span = pl.ds(first, count)
        left = remote(
            field.at[span, pl.ds(BASE, HALO)], field.at[span, pl.ds(BASE + tile_cols, HALO)],
            send.at[at], recv.at[at], col=jnp.maximum(me_c - 1, 0),
        )
        right = remote(
            field.at[span, pl.ds(BASE + tile_cols - HALO, HALO)], field.at[span, pl.ds(PAD, HALO)],
            send.at[at + 1], recv.at[at + 1], col=jnp.minimum(me_c + 1, n_col - 1),
        )
        return left, right

    def start(pair, first_ok, second_ok):
        pl.when(first_ok)(lambda: pair[0].start())
        pl.when(second_ok)(lambda: pair[1].start())

    def wait_recv(pair, first_ok, second_ok):
        pl.when(second_ok)(lambda: pair[0].wait_recv())
        pl.when(first_ok)(lambda: pair[1].wait_recv())

    def wait_send(pair, first_ok, second_ok):
        pl.when(first_ok)(lambda: pair[0].wait_send())
        pl.when(second_ok)(lambda: pair[1].wait_send())

    half = prod.shape[1] // 2
    firsts = []
    for k, to in enumerate(targets):
        loads[k].wait()
        product = jnp.dot(res_ref[...], bins[k], preferred_element_type=jnp.float32)
        for h in range(2):
            mark = touched_ref[0, 0, 2 * to + h].astype(jnp.float32)
            prod[2 * to + h] = product[:, h * tile_cols:(h + 1) * tile_cols] * mark
        if k == 0:
            pl.semaphore_wait(barrier, n_col - 1 + n_row - 1)
        for h in range(2):
            part = pl.ds(h * half, half)
            copy = remote(
                prod.at[2 * to + 1 - b, part], recv1.at[to, part], s1.at[to, h], r1.at[to, h], col=peer
            )
            copy.start()
            firsts.append(copy)

    img_rows = row_copies(
        image_ref.at[pl.ds(0, HALO)], image_ref.at[pl.ds(tile_rows - HALO, HALO)],
        halo_img, img_send, img_recv,
    )
    start(img_rows, up_ok, down_ok)
    for j in range(tiles):
        rows = pl.ds(j * LANES, LANES)
        img_t[j, main, :] = image_ref[rows, :].T
        prec_t[j] = precond_ref[rows, :].T
    img_cols = col_copies(img_t, 0, tiles, 2, img_send, img_recv)
    start(img_cols, left_ok, right_ok)

    strip_top = strip_ref[:, :LANES].astype(jnp.float32).T[:HALO]
    strip_bottom = strip_ref[:, tile_rows - LANES:].astype(jnp.float32).T[LANES - HALO:]
    strip_edges = jnp.concatenate([strip_top, strip_bottom], 0).astype(jnp.bfloat16)

    depth = img_t.shape[1]
    lane = lax.broadcasted_iota(jnp.int32, (depth, LANES), 1)
    col_ids = me_c * tile_cols - BASE + lax.broadcasted_iota(jnp.int32, (depth, LANES), 0)
    for j in range(tiles + 1):
        if j < tiles:
            row_ids = me_r * tile_rows + j * LANES + lane
        else:
            row_ids = me_r * tile_rows + jnp.where(lane < LANES // 2, tile_rows + lane, lane - LANES)
        inside = (row_ids >= 0) & (row_ids < total_rows) & (col_ids >= 0) & (col_ids < total_cols)
        mask_d[j] = jnp.where(inside & (row_ids < total_rows - 1), dual_step, 0.0)
        mask_r[j] = jnp.where(inside & (col_ids < total_cols - 1), dual_step, 0.0)

    seconds = []
    for k, to in enumerate(targets[:-1]):
        for h in range(2):
            part = pl.ds(h * half, half)
            firsts[2 * k + h].wait_recv()
            send2[to, part] = prod[2 * to + b, part] + recv1[to, part]
            copy = remote(
                send2.at[to, part], recv2.at[g, part], s2.at[to, h], r2.at[g, h], col=2 * to + b
            )
            copy.start()
            seconds.append(copy)

    wait_recv(img_rows, up_ok, down_ok)
    img_t[tiles, main, :] = halo_img[...].T
    img_corner = col_copies(img_t, tiles, 1, 4, img_send, img_recv)
    start(img_corner, left_ok, right_ok)

    for copy in firsts[-2:]:
        copy.wait_recv()
    sums = prod[2 * g + b] + recv1[g]
    for d in range(1, groups):
        sender = lax.rem(g + d, groups)
        for h in range(2):
            part = pl.ds(h * half, half)
            remote(
                send2.at[sender, part], recv2.at[sender, part], s2.at[sender, h], r2.at[sender, h], col=peer
            ).wait_recv()
        sums = sums + recv2[sender]

    def parts(x):
        high = x.astype(jnp.bfloat16)
        return high, (x - high.astype(jnp.float32)).astype(jnp.bfloat16)

    high, low = parts(sums)
    edges = jnp.dot(strip_edges, high, preferred_element_type=jnp.float32)
    edges = edges + jnp.dot(strip_edges, low, preferred_element_type=jnp.float32)
    strips[pl.ds(0, HALO), :] = edges[:HALO] * precond_ref[pl.ds(0, HALO), :]
    strips[pl.ds(HALO, HALO), :] = edges[HALO:] * precond_ref[pl.ds(tile_rows - HALO, HALO), :]
    step_rows = row_copies(
        strips.at[pl.ds(0, HALO)], strips.at[pl.ds(HALO, HALO)], halo_step, step_send, step_recv
    )
    start(step_rows, up_ok, down_ok)

    high, low = parts(sums.T)
    square = jnp.zeros((8, LANES), jnp.float32)
    for j in range(tiles):
        weights = strip_ref[:, j * LANES:(j + 1) * LANES]
        grad = jnp.dot(high, weights, preferred_element_type=jnp.float32)
        grad = grad + jnp.dot(low, weights, preferred_element_type=jnp.float32)
        step = prec_t[j] * grad
        step_t[j, main, :] = step
        square = square + jnp.sum((step * step).reshape(tile_cols // 8, 8, LANES), 0)

    def spread_over(value, slots, mine, count, axis, send, recv):
        slots[mine] = value
        copies = []
        for d in range(1, count):
            to = lax.rem(mine + d, count)
            copy = remote(slots.at[mine], slots.at[mine], send.at[to], recv.at[mine], **{axis: to})
            copy.start()
            copies.append(copy)
        return copies

    def collected(slots, mine, count, axis, send, recv):
        for d in range(1, count):
            at = lax.rem(mine + d, count)
            remote(slots.at[at], slots.at[at], send.at[at], recv.at[at], **{axis: at}).wait_recv()
        total = slots[0]
        for i in range(1, count):
            total = total + slots[i]
        return total

    pending = spread_over(square, sq_row, me_r, n_row, "row", sq_row_s, sq_row_r)
    step_cols = col_copies(step_t, 0, tiles, 2, step_send, step_recv)
    start(step_cols, left_ok, right_ok)
    wait_recv(step_rows, up_ok, down_ok)
    step_t[tiles, main, :] = halo_step[...].T
    step_corner = col_copies(step_t, tiles, 1, 4, step_send, step_recv)
    start(step_corner, left_ok, right_ok)
    square = collected(sq_row, me_r, n_row, "row", sq_row_s, sq_row_r)
    pending += spread_over(square, sq_col, me_c, n_col, "col", sq_col_s, sq_col_r)
    for pair in (img_cols, img_corner, step_cols, step_corner):
        wait_recv(pair, left_ok, right_ok)
    square = collected(sq_col, me_c, n_col, "col", sq_col_s, sq_col_r)
    spread = jnp.sqrt(jnp.sum(square, axis=(0, 1), keepdims=True) / cell_total + epsilon)
    factor = jnp.minimum(1.0, radius / spread)
    factor = jnp.broadcast_to(factor, (depth, LANES))
    for j in range(tiles + 1):
        scaled_ref[j] = (img_t[j] - factor * step_t[j]) / tv_weight

    def turned(pieces, shift):
        rolled = [pltpu.roll(piece, shift % LANES, 1) for piece in pieces]
        at = lax.broadcasted_iota(jnp.int32, pieces[0].shape, 1)
        edge = at == (0 if shift > 0 else LANES - 1)
        n = len(pieces)
        return [jnp.where(edge, rolled[(i - shift) % n], rolled[i]) for i in range(n)]

    every = range(tiles + 1)

    def divergence(first, size, count=tiles + 1):
        p = [p_ref[j, pl.ds(first, size), :] for j in every]
        above = turned(p, 1)
        q = [q_ref[j, pl.ds(first, size), :] for j in range(count)]
        beside = [q_ref[j, pl.ds(first - 1, size), :] for j in range(count)]
        return [p[j] - above[j] + (q[j] - beside[j]) for j in range(count)]

    CHUNK = 16

    def turn(low_end, high_end):
        for first in range(low_end, high_end, CHUNK):
            div = divergence(first, CHUNK)
            for j in every:
                pot_ref[j, pl.ds(first, CHUNK), :] = div[j] - scaled_ref[j, pl.ds(first, CHUNK), :]
        for first in range(low_end, high_end, CHUNK):
            here = pl.ds(first, CHUNK)
            pot = [pot_ref[j, here, :] for j in every]
            below = turned(pot, -1)
            for j in every:
                grad_d = (below[j] - pot[j]) * mask_d[j, here, :]
                grad_r = (pot_ref[j, pl.ds(first + 1, CHUNK), :] - pot[j]) * mask_r[j, here, :]
                inverse = 1.0 / (1.0 + jnp.sqrt(grad_d * grad_d + grad_r * grad_r))
                p_ref[j, here, :] = (p_ref[j, here, :] + grad_d) * inverse
                q_ref[j, here, :] = (q_ref[j, here, :] + grad_r) * inverse

    wide = max(0, ITERS - PAD)

    @pl.loop(0, wide)
    def _(_):
        turn(PAD, depth - PAD)

    @pl.loop(wide, ITERS)
    def _(_):
        turn(HALO, depth - HALO)

    moved = jnp.zeros((8, LANES), jnp.float32)
    for first in range(BASE, BASE + tile_cols, CHUNK):
        div = divergence(first, CHUNK, tiles)
        for j in range(tiles):
            here = pl.ds(first, CHUNK)
            updated = tv_weight * (scaled_ref[j, here, :] - div[j])
            pot_ref[j, here, :] = updated
            change = updated - img_t[j, here, :]
            moved = moved + jnp.sum((change * change).reshape(CHUNK // 8, 8, LANES), 0)
    pending += spread_over(moved, ch_row, me_r, n_row, "row", ch_row_s, ch_row_r)
    moved = collected(ch_row, me_r, n_row, "row", ch_row_s, ch_row_r)
    pending += spread_over(moved, ch_col, me_c, n_col, "col", ch_col_s, ch_col_r)
    for j in range(tiles):
        out_ref[pl.ds(j * LANES, LANES), :] = pot_ref[j, main, :].T
    for copy in firsts + seconds:
        copy.wait_send()
    for pair in (img_rows, step_rows):
        wait_send(pair, up_ok, down_ok)
    for pair in (img_cols, img_corner, step_cols, step_corner):
        wait_send(pair, left_ok, right_ok)
    moved = collected(ch_col, me_c, n_col, "col", ch_col_s, ch_col_r)
    mean_ref[0] = jnp.sum(moved) / cell_total
    for copy in pending:
        copy.wait_send()


def solution(mesh):
    n_row, n_col = mesh.shape["row"], mesh.shape["col"]

    def local(residual, strip_weights, bin_weights, touched, image, precond):
        angles = residual.shape[0]
        tile_rows, tile_cols = image.shape
        tiles = tile_rows // LANES
        depth = tile_cols + 2 * BASE
        groups = n_col // 2
        f32 = jnp.float32
        vmem = pl.BlockSpec(memory_space=pltpu.VMEM)
        smem = pl.BlockSpec(memory_space=pltpu.SMEM)
        dma = pltpu.SemaphoreType.DMA
        field = pltpu.VMEM((tiles + 1, depth, LANES), f32)
        strip = pltpu.VMEM((LANES, tile_cols), f32)
        updated, mean_change = pl.pallas_call(
            functools.partial(kernel, n_row, n_col),
            out_shape=(
                jax.ShapeDtypeStruct(image.shape, f32),
                jax.ShapeDtypeStruct((1,), f32),
            ),
            in_specs=[vmem, vmem, pl.BlockSpec(memory_space=pl.ANY), smem, vmem, vmem],
            out_specs=(vmem, smem),
            scratch_shapes=[
                pltpu.VMEM((n_col, angles, tile_cols), f32),
                pltpu.VMEM((groups, angles, tile_cols), f32),
                pltpu.VMEM((groups, angles, tile_cols), f32),
                pltpu.VMEM((groups, angles, tile_cols), f32),
                field, field, strip, strip,
                pltpu.VMEM((2 * HALO, tile_cols), f32),
                pltpu.VMEM((tiles, tile_cols, LANES), f32),
                field, field, field, field, field, field,
                pltpu.VMEM((n_row, 8, LANES), f32),
                pltpu.VMEM((n_col, 8, LANES), f32),
                pltpu.VMEM((n_row, 8, LANES), f32),
                pltpu.VMEM((n_col, 8, LANES), f32),
                dma((groups, 2)), dma((groups, 2)), dma((groups, 2)), dma((groups, 2)),
                pltpu.VMEM((groups, bin_weights.shape[1], 2 * tile_cols), bin_weights.dtype), dma((groups,)),
                dma((6,)), dma((6,)), dma((6,)), dma((6,)),
                dma((n_row,)), dma((n_row,)), dma((n_col,)), dma((n_col,)),
                dma((n_row,)), dma((n_row,)), dma((n_col,)), dma((n_col,)),
            ],
            compiler_params=pltpu.CompilerParams(collective_id=0, has_side_effects=True),
            name="tv_step",
        )(residual, strip_weights, bin_weights, touched, image, precond)
        return updated, mean_change.reshape(())

    in_specs = (
        P("row", "col"),
        P("row", None),
        P("row", "col", None),
        P("row", "col", None),
        P("row", "col"),
        P("row", "col"),
    )
    return jax.shard_map(
        local, mesh=mesh, in_specs=in_specs, out_specs=(P("row", "col"), P()), check_vma=False
    )
```
